32 devices in a mesh: seg: 4 (over z), ch: 8 (over y, x, core).
Axes of the slice: x: 2, y: 2, z: 4, core: 2. Of those that a mesh axis runs over, the one named last changes fastest.
Arguments:
- gate_in: bfloat16 [1536, 16384], P('ch', 'seg'), may hold values from -6 to 6
- key_in: bfloat16 [1536, 16384], P('ch', 'seg'), may hold values from -6 to 6
- value_in: bfloat16 [1536, 16384], P('ch', 'seg'), may hold values from -6 to 6
- kernel: float32 [1536, 16384], P('ch'), may hold values from -0.046875 to 0.046875
- skip_gain: float32 [1536], P('ch'), may hold values from -1 to 1
- out_weight: bfloat16 [1536, 1536], P('ch'), may hold values from -0.15625 to 0.15625
Outputs:
- output: bfloat16 [16384, 1536], P(('seg', 'ch'))
The draws below stay inside these ranges and needn't reach their ends.
All inputs are finite; a program needn't handle non-finite values.
Results may differ from the reference program's by a relative error of at most 0.0095.
Values may be sent and summed in bfloat16 or wider, within the bound.
No kernel may reach another device: no remote copies, remote signals or barrier semaphores. Data moves between devices by JAX's collectives and lax.ppermute only.
A program may use at most 128 MiB of HBM per device.

```python
import jax
import jax.numpy as jnp
from jax import lax

D = 1536
SEQ = 16384


def level_of(rng, extent, cuts, least, top_value):
    level = 1.0
    for axis_at, shards_of in cuts:
        heights = jax.random.uniform(jax.random.fold_in(jax.random.fold_in(rng, 6), axis_at), (shards_of,), jnp.float32, least / len(cuts), top_value / len(cuts))
        level = level * jnp.repeat(jnp.exp(heights), extent[axis_at] // shards_of).reshape((-1,) + (1,) * (len(extent) - 1 - axis_at))
    return level


def bell_draw(key, extent, deviation, bound, split=(), dtype=jnp.bfloat16):
    drawn = deviation * jax.random.normal(key, extent, jnp.float32)
    if split:
        drawn = drawn * level_of(key, extent, split, -0.22, 0.18)
    return jnp.clip(drawn, -bound, bound).astype(dtype)


def setup_inputs(seed: int = 0) -> dict:
    key_list = jax.random.split(jax.random.key(seed), 7)
    gate_in = bell_draw(key_list[0], (D, SEQ), 1.0, 6.0, ((0, 8), (1, 4)))
    key_in = bell_draw(key_list[1], (D, SEQ), 1.0, 6.0, ((0, 8), (1, 4)))
    value_in = bell_draw(key_list[2], (D, SEQ), 1.0, 6.0, ((0, 8), (1, 4)))
    kernel = bell_draw(key_list[3], (D, SEQ), SEQ ** -0.5, 0.046875, ((0, 8),), jnp.float32)
    skip_gain = jnp.clip(jax.random.uniform(key_list[4], (D,), jnp.float32, -1.0, 1.0) * level_of(key_list[4], (D,), ((0, 8),), -0.4, 0.0), -1.0, 1.0)
    out_weight = bell_draw(key_list[5], (D, D), D ** -0.5, 0.15625, ((0, 8),))
    return dict(gate_in=gate_in, key_in=key_in, value_in=value_in, kernel=kernel, skip_gain=skip_gain, out_weight=out_weight)


def reference(gate_in, key_in, value_in, kernel, skip_gain, out_weight):
    mixed_in = key_in.astype(jnp.float32) * value_in.astype(jnp.float32)
    length = mixed_in.shape[1]
    product = jnp.fft.rfft(mixed_in, n=2 * length, axis=1) * jnp.fft.rfft(kernel, n=2 * length, axis=1)
    convolved = jnp.fft.irfft(product, n=2 * length, axis=1)[:, :length]
    gated = (gate_in.astype(jnp.float32) * (convolved + skip_gain[:, None] * mixed_in)).astype(jnp.bfloat16)
    result = lax.dot_general(gated, out_weight, (((0,), (0,)), ((), ())), preferred_element_type=jnp.float32)
    return result.astype(jnp.bfloat16)
```

```python
import math
from functools import partial

import jax
import jax.numpy as jnp
import numpy as np
from jax import lax
from jax.experimental import pallas as pl
from jax.experimental.pallas import tpu as pltpu
from jax.sharding import PartitionSpec as P

lane_width = 128
row_pad = 8
f32 = jnp.float32
bf16 = jnp.bfloat16


def make_tables(rows):
    length = rows * lane_width
    k1 = np.arange(rows)[:, None] + 0.25
    outer = 2.0 * math.pi * (k1 * np.arange(rows)[None, :]) / rows
    twist = 2.0 * math.pi * (k1 * np.arange(lane_width)[None, :]) / length
    lanes = np.arange(lane_width)
    inner = 2.0 * math.pi * (lanes[:, None] * lanes[None, :] % lane_width) / lane_width
    cos_i, sin_i = np.cos(inner), np.sin(inner)
    outer_fwd = np.concatenate([np.cos(outer), -np.sin(outer)], 0)
    inner_fwd = np.block([[cos_i, -sin_i], [sin_i, cos_i]])
    inner_inv = np.block([[cos_i, sin_i], [-sin_i, cos_i]])
    outer_inv = np.concatenate([np.cos(outer.T), -np.sin(outer.T)], 1) / length
    mats = tuple(jnp.asarray(m, dtype=bf16) for m in (outer_fwd, inner_fwd, inner_inv, outer_inv))
    return mats, (jnp.asarray(np.cos(twist), f32), jnp.asarray(-np.sin(twist), f32))


def mm(a, b):
    return jnp.dot(a, b, preferred_element_type=f32)


def forward(read, members, rows, outer_fwd, inner_fwd, tw_re, tw_im):
    side = jnp.concatenate([read(g) for g in members], axis=1).astype(bf16)
    a = mm(outer_fwd, side)
    parts = []
    for i in range(len(members)):
        re = a[:rows, i * lane_width : (i + 1) * lane_width]
        im = a[rows:, i * lane_width : (i + 1) * lane_width]
        parts.append(jnp.concatenate([re * tw_re - im * tw_im, re * tw_im + im * tw_re], axis=1))
    return mm(jnp.concatenate(parts, axis=0).astype(bf16), inner_fwd)


def members_of(count):
    width = 2 if count % 2 == 0 else 1
    return [tuple(range(g, g + width)) for g in range(0, count, width)]


def filter_body(rows, count, k_ref, of_ref, if_ref, tr_ref, ti_ref, out_ref, rows_s):
    pitch = rows + row_pad
    for r in range(rows):
        rows_s[pl.ds(r, count, stride=pitch), :] = k_ref[:, r * lane_width : (r + 1) * lane_width]
    read = lambda g: rows_s[pl.ds(g * pitch, rows), :]
    for members in members_of(count):
        spec = forward(read, members, rows, of_ref[...], if_ref[...], tr_ref[...], ti_ref[...])
        out_ref[pl.ds(members[0] * rows, len(members) * rows), :] = spec


def conv_body(rows, count, segs, u_ref, h_ref, of_ref, if_ref, ii_ref, oi_ref, tr_ref, ti_ref, out_ref, in_s, out_s):
    pitch = rows + row_pad
    per = rows // segs
    for r in range(rows):
        s, q = divmod(r, per)
        in_s[pl.ds(r, count, stride=pitch), :] = u_ref[s, :, q * lane_width : (q + 1) * lane_width].astype(f32)
    read = lambda g: in_s[pl.ds(g * pitch, rows), :]
    tw_re, tw_im = tr_ref[...], ti_ref[...]
    for members in members_of(count):
        x = forward(read, members, rows, of_ref[...], if_ref[...], tw_re, tw_im)
        h = h_ref[pl.ds(members[0] * rows, len(members) * rows), :]
        xr, xi = x[:, :lane_width], x[:, lane_width:]
        hr, hi = h[:, :lane_width], h[:, lane_width:]
        prod = jnp.concatenate([hr * xr - hi * xi, hr * xi + hi * xr], axis=1).astype(bf16)
        c = mm(prod, ii_ref[...])
        cols = []
        for i in range(len(members)):
            cr = c[i * rows : (i + 1) * rows, :lane_width]
            ci = c[i * rows : (i + 1) * rows, lane_width:]
            cols.append(jnp.concatenate([cr * tw_re + ci * tw_im, ci * tw_re - cr * tw_im], axis=0))
        y = mm(oi_ref[...], jnp.concatenate(cols, axis=1).astype(bf16))
        for i, g in enumerate(members):
            out_s[pl.ds(g * pitch, rows), :] = y[:, i * lane_width : (i + 1) * lane_width]
    for r in range(rows):
        s, q = divmod(r, per)
        out_ref[s, :, q * lane_width : (q + 1) * lane_width] = out_s[pl.ds(r, count, stride=pitch), :].astype(bf16)


def whole(array):
    return pl.BlockSpec(array.shape, lambda *_: (0,) * array.ndim)


def filter_call(my_kernel, step, chunk, mats, twists):
    full = my_kernel.shape[1]
    rows = full // lane_width
    consts = (mats[0], mats[1], *twists)
    return pl.pallas_call(
        partial(filter_body, rows, step),
        grid=(1,),
        in_specs=[pl.BlockSpec((step, full), lambda i: (chunk, 0)), *map(whole, consts)],
        out_specs=pl.BlockSpec((step * rows, 2 * lane_width), lambda i: (i, 0)),
        out_shape=jax.ShapeDtypeStruct((step * rows, 2 * lane_width), f32),
        scratch_shapes=[pltpu.VMEM((step * (rows + row_pad), lane_width), f32)],
        compiler_params=pltpu.CompilerParams(vmem_limit_bytes=40 << 20),
        cost_estimate=pl.CostEstimate(flops=step * rows * 3 * rows * 4 * lane_width, transcendentals=0, bytes_accessed=step * full * 12),
        name="filter_spectrum",
    )(my_kernel, *consts)


def conv_call(streams, spectrum, mats, twists):
    segs, step, part = streams.shape
    full = segs * part
    rows = full // lane_width
    consts = (*mats, *twists)
    pad_rows = step * (rows + row_pad)
    return pl.pallas_call(
        partial(conv_body, rows, step, segs),
        grid=(1,),
        in_specs=[
            pl.BlockSpec((segs, step, part), lambda i: (0, 0, 0)),
            pl.BlockSpec((step * rows, 2 * lane_width), lambda i: (0, 0)),
            *map(whole, consts),
        ],
        out_specs=pl.BlockSpec((segs, step, part), lambda i: (0, 0, 0)),
        out_shape=jax.ShapeDtypeStruct((segs, step, part), bf16),
        scratch_shapes=[pltpu.VMEM((pad_rows, lane_width), f32), pltpu.VMEM((pad_rows, lane_width), f32)],
        compiler_params=pltpu.CompilerParams(vmem_limit_bytes=40 << 20),
        cost_estimate=pl.CostEstimate(flops=step * rows * 6 * rows * 4 * lane_width, transcendentals=0, bytes_accessed=step * full * 12),
        name="long_conv",
    )(streams, spectrum, *consts)


def on_device(gate_in, key_in, value_in, kernel, skip_gain, out_weight):
    segs = lax.axis_size("seg")
    groups = lax.axis_size("ch")
    held, part = key_in.shape
    full = kernel.shape[1]
    width = out_weight.shape[1]
    col = held // segs
    step = 16 if col % 16 == 0 else col
    chunks = col // step
    mats, twists = make_tables(full // lane_width)

    def cut(array):
        return array.reshape(segs, chunks, step, *array.shape[1:])

    key_c, value_c, gate_c, skip_c = map(cut, (key_in, value_in, gate_in, skip_gain))

    def mixed(j):
        return key_c[:, j].astype(f32) * value_c[:, j].astype(f32)

    swap = partial(lax.all_to_all, split_axis=0, concat_axis=0, tiled=True)
    arrived = [swap(mixed(j).astype(bf16), "seg") for j in range(chunks)]
    my_kernel = lax.dynamic_slice_in_dim(kernel, lax.axis_index("seg") * col, col, 0)
    spectra = [filter_call(my_kernel, step, j, mats, twists) for j in range(chunks)]
    weights = lax.all_gather(out_weight, "ch", axis=0, tiled=True)
    weights = weights.reshape(groups, segs, chunks, step, width)
    result = None
    for j in range(chunks):
        convolved = swap(conv_call(arrived[j], spectra[j], mats, twists), "seg")
        gated = (
            gate_c[:, j].astype(f32) * (convolved.astype(f32) + skip_c[:, j, :, None] * mixed(j))
        ).astype(bf16)
        tokens = gated.reshape(segs * step, groups, part // groups).transpose(1, 0, 2)
        mine = swap(tokens, "ch").reshape(groups * segs * step, part // groups)
        share = lax.dot_general(
            mine,
            weights[:, :, j].reshape(groups * segs * step, width),
            (((0,), (0,)), ((), ())),
            preferred_element_type=f32,
        )
        result = share if result is None else result + share
    return result.astype(bf16)


def solution(mesh):
    placed = (P("ch", "seg"), P("ch", "seg"), P("ch", "seg"), P("ch", None), P("ch"), P("ch", None))
    return jax.shard_map(
        on_device, mesh=mesh, in_specs=placed, out_specs=P(("seg", "ch"), None), check_vma=False
    )
```

```python
import math
from functools import partial

import jax
import jax.numpy as jnp
import numpy as np
from jax import lax
from jax.experimental import pallas as pl
from jax.experimental.pallas import tpu as pltpu
from jax.sharding import PartitionSpec as P

lane_width = 128
row_pad = 8
f32 = jnp.float32
bf16 = jnp.bfloat16


def make_tables(rows):
    length = rows * lane_width
    k1 = np.arange(rows)[:, None] + 0.25
    outer = 2.0 * math.pi * (k1 * np.arange(rows)[None, :]) / rows
    twist = 2.0 * math.pi * (k1 * np.arange(lane_width)[None, :]) / length
    lanes = np.arange(lane_width)
    inner = 2.0 * math.pi * (lanes[:, None] * lanes[None, :] % lane_width) / lane_width
    cos_i, sin_i = np.cos(inner), np.sin(inner)
    outer_fwd = np.concatenate([np.cos(outer), -np.sin(outer)], 0)
    inner_fwd = np.block([[cos_i, -sin_i], [sin_i, cos_i]])
    inner_inv = np.block([[cos_i, sin_i], [-sin_i, cos_i]])
    outer_inv = np.concatenate([np.cos(outer.T), -np.sin(outer.T)], 1) / length
    mats = tuple(jnp.asarray(m, dtype=bf16) for m in (outer_fwd, inner_fwd, inner_inv, outer_inv))
    return mats, (jnp.asarray(np.cos(twist), f32), jnp.asarray(-np.sin(twist), f32))


def mm(a, b):
    return jnp.dot(a, b, preferred_element_type=f32)


def forward(read, members, rows, outer_fwd, inner_fwd, tw_re, tw_im):
    side = jnp.concatenate([read(g) for g in members], axis=1).astype(bf16)
    a = mm(outer_fwd, side)
    parts = []
    for i in range(len(members)):
        re = a[:rows, i * lane_width : (i + 1) * lane_width]
        im = a[rows:, i * lane_width : (i + 1) * lane_width]
        parts.append(jnp.concatenate([re * tw_re - im * tw_im, re * tw_im + im * tw_re], axis=1))
    return mm(jnp.concatenate(parts, axis=0).astype(bf16), inner_fwd)


def members_of(count):
    width = 2 if count % 2 == 0 else 1
    return [tuple(range(g, g + width)) for g in range(0, count, width)]


def filter_body(rows, count, k_ref, of_ref, if_ref, tr_ref, ti_ref, out_ref, rows_s):
    pitch = rows + row_pad
    for r in range(rows):
        rows_s[pl.ds(r, count, stride=pitch), :] = k_ref[:, r * lane_width : (r + 1) * lane_width]
    read = lambda g: rows_s[pl.ds(g * pitch, rows), :]
    for members in members_of(count):
        spec = forward(read, members, rows, of_ref[...], if_ref[...], tr_ref[...], ti_ref[...])
        out_ref[pl.ds(members[0] * rows, len(members) * rows), :] = spec


def conv_body(rows, count, segs, me_ref, *refs):
    u_refs, refs = refs[:segs], refs[segs:]
    h_ref, of_ref, if_ref, ii_ref, oi_ref, tr_ref, ti_ref, *refs = refs
    out_refs, (in_s, out_s) = refs[:segs], refs[segs:]
    pitch = rows + row_pad
    per = rows // segs
    me = me_ref[0]
    for d in range(segs):
        base = lax.rem(me + (segs - d), segs) * per
        for q in range(per):
            in_s[pl.ds(base + q, count, stride=pitch), :] = u_refs[d][:, q * lane_width : (q + 1) * lane_width].astype(f32)
    read = lambda g: in_s[pl.ds(g * pitch, rows), :]
    tw_re, tw_im = tr_ref[...], ti_ref[...]
    for members in members_of(count):
        x = forward(read, members, rows, of_ref[...], if_ref[...], tw_re, tw_im)
        h = h_ref[pl.ds(members[0] * rows, len(members) * rows), :]
        xr, xi = x[:, :lane_width], x[:, lane_width:]
        hr, hi = h[:, :lane_width], h[:, lane_width:]
        prod = jnp.concatenate([hr * xr - hi * xi, hr * xi + hi * xr], axis=1).astype(bf16)
        c = mm(prod, ii_ref[...])
        cols = []
        for i in range(len(members)):
            cr = c[i * rows : (i + 1) * rows, :lane_width]
            ci = c[i * rows : (i + 1) * rows, lane_width:]
            cols.append(jnp.concatenate([cr * tw_re + ci * tw_im, ci * tw_re - cr * tw_im], axis=0))
        y = mm(oi_ref[...], jnp.concatenate(cols, axis=1).astype(bf16))
        for i, g in enumerate(members):
            out_s[pl.ds(g * pitch, rows), :] = y[:, i * lane_width : (i + 1) * lane_width]
    for d in range(segs):
        base = lax.rem(me + d, segs) * per
        for q in range(per):
            out_refs[d][:, q * lane_width : (q + 1) * lane_width] = out_s[pl.ds(base + q, count, stride=pitch), :].astype(bf16)


def whole(array):
    return pl.BlockSpec(array.shape, lambda *_: (0,) * array.ndim)


def filter_call(my_kernel, step, chunk, mats, twists):
    full = my_kernel.shape[1]
    rows = full // lane_width
    consts = (mats[0], mats[1], *twists)
    return pl.pallas_call(
        partial(filter_body, rows, step),
        grid=(1,),
        in_specs=[pl.BlockSpec((step, full), lambda i: (chunk, 0)), *map(whole, consts)],
        out_specs=pl.BlockSpec((step * rows, 2 * lane_width), lambda i: (i, 0)),
        out_shape=jax.ShapeDtypeStruct((step * rows, 2 * lane_width), f32),
        scratch_shapes=[pltpu.VMEM((step * (rows + row_pad), lane_width), f32)],
        compiler_params=pltpu.CompilerParams(vmem_limit_bytes=40 << 20),
        cost_estimate=pl.CostEstimate(flops=step * rows * 3 * rows * 4 * lane_width, transcendentals=0, bytes_accessed=step * full * 12),
        name="filter_spectrum",
    )(my_kernel, *consts)


def conv_call(me, streams, spectrum, mats, twists):
    segs = len(streams)
    step, part = streams[0].shape
    full = segs * part
    rows = full // lane_width
    consts = (*mats, *twists)
    pad_rows = step * (rows + row_pad)
    block = pl.BlockSpec((step, part), lambda i: (0, 0))
    return pl.pallas_call(
        partial(conv_body, rows, step, segs),
        grid=(1,),
        in_specs=[
            pl.BlockSpec(memory_space=pltpu.SMEM),
            *[block] * segs,
            pl.BlockSpec((step * rows, 2 * lane_width), lambda i: (0, 0)),
            *map(whole, consts),
        ],
        out_specs=[block] * segs,
        out_shape=[jax.ShapeDtypeStruct((step, part), bf16)] * segs,
        scratch_shapes=[pltpu.VMEM((pad_rows, lane_width), f32), pltpu.VMEM((pad_rows, lane_width), f32)],
        compiler_params=pltpu.CompilerParams(vmem_limit_bytes=40 << 20),
        cost_estimate=pl.CostEstimate(flops=step * rows * 6 * rows * 4 * lane_width, transcendentals=0, bytes_accessed=step * full * 12),
        name="long_conv",
    )(me.reshape(1), *streams, spectrum, *consts)


def send_round(blocks, axis):
    count = len(blocks)
    return [
        blocks[d] if d == 0 else lax.ppermute(blocks[d], axis, [(i, (i + d) % count) for i in range(count)])
        for d in range(count)
    ]


def gather_all(block, axis):
    count = lax.axis_size(axis)
    bits = count.bit_length() - 1
    if count != 1 << bits:
        return lax.all_gather(block, axis, axis=0, tiled=False)
    me = lax.axis_index(axis)
    held = block.reshape((1,) * bits + block.shape)
    for bit in (*range(1, bits), 0):
        theirs = lax.ppermute(held, axis, [(i, i ^ (1 << bit)) for i in range(count)])
        low = (me >> bit) % 2 == 0
        held = jnp.concatenate([jnp.where(low, held, theirs), jnp.where(low, theirs, held)], axis=bits - 1 - bit)
    return held.reshape(count, *block.shape)


def on_device(gate_in, key_in, value_in, kernel, skip_gain, out_weight):
    segs = lax.axis_size("seg")
    groups = lax.axis_size("ch")
    me = lax.axis_index("seg")
    held, part = key_in.shape
    full = kernel.shape[1]
    width = out_weight.shape[1]
    col = held // segs
    step = col // 2 if col % (8 * 2) == 0 else col
    chunks = col // step
    mats, twists = make_tables(full // lane_width)

    def take(array, group, j):
        return lax.dynamic_slice_in_dim(array, group * col + j * step, step, 0)

    def mixed(group, j):
        return take(key_in, group, j).astype(f32) * take(value_in, group, j).astype(f32)

    ups = [lax.rem(me + d, segs) for d in range(segs)]
    downs = [lax.rem(me + (segs - d), segs) for d in range(segs)]
    arrived = []
    for j in range(chunks):
        with jax.named_scope(f"out_{j}"):
            arrived.append(send_round([mixed(g, j).astype(bf16) for g in ups], "seg"))
    my_kernel = lax.dynamic_slice_in_dim(kernel, me * col, col, 0)
    spectra = [filter_call(my_kernel, step, j, mats, twists) for j in range(chunks)]
    swap = partial(lax.all_to_all, split_axis=0, concat_axis=0, tiled=True)
    ordered = jnp.stack([jnp.concatenate([take(out_weight, g, j) for g in downs], 0) for j in range(chunks)])
    with jax.named_scope("weights"):
        weights = gather_all(ordered, "ch")
    tokens = []
    for j in range(chunks):
        with jax.named_scope(f"back_{j}"):
            back = send_round(conv_call(me, arrived[j], spectra[j], mats, twists), "seg")
        tokens += [
            (take(gate_in, g, j).astype(f32) * (y.astype(f32) + take(skip_gain, g, j)[:, None] * mixed(g, j))).astype(bf16)
            for g, y in zip(downs, back)
        ]
    tokens = jnp.concatenate(tokens, 0).reshape(held, groups, part // groups).transpose(1, 0, 2)
    mine = swap(tokens, "ch").reshape(groups * held, part // groups)
    result = lax.dot_general(
        mine, weights.reshape(groups * held, width), (((0,), (0,)), ((), ())), preferred_element_type=f32
    )
    return result.astype(bf16)


def solution(mesh):
    placed = (P("ch", "seg"), P("ch", "seg"), P("ch", "seg"), P("ch", None), P("ch"), P("ch", None))
    return jax.shard_map(
        on_device, mesh=mesh, in_specs=placed, out_specs=P(("seg", "ch"), None), check_vma=False
    )
```
